32 devices in a mesh: rep: 4 (over z), row: 2 (over x), col: 4 (over y, core).
Axes of the slice: x: 2, y: 2, z: 4, core: 2. Of those that a mesh axis runs over, the one named last changes fastest.
Arguments:
- grad_parts: bfloat16 [4, 8192, 8192], P('rep', 'row', 'col'), may hold values from -6 to 6
- momentum: float32 [8192, 8192], P(('row', 'rep'), 'col'), may hold values from -24 to 24
- basis: float32 [8192, 384], P('col'), may hold values from -0.0625 to 0.0625
Outputs:
- update: bfloat16 [8192, 8192], P('row', 'col')
- new_momentum: float32 [8192, 8192], P(('row', 'rep'), 'col')
- new_basis: float32 [8192, 384], P('col')
- power_norms: float32 [384], replicated
The draws below stay inside these ranges and needn't reach their ends.
All inputs are finite; a program needn't handle non-finite values.
Results may differ from the reference program's by a relative error of at most 0.0085.
Values may be sent and summed in bfloat16 or wider, within the bound.
No kernel may reach another device: no remote copies, remote signals or barrier semaphores. Data moves between devices by JAX's collectives and lax.ppermute only.
A program may use at most 128 MiB of HBM per device.

```python
import jax
import jax.numpy as jnp
from jax import lax

D = 8192
RANK = 384
REPLICAS = 4


def draw_momentum(key, part):
    first = jax.random.fold_in(key, 101)
    second = jax.random.fold_in(key, 202)
    position = jnp.arange(D, dtype=jnp.float32) / (D - 1)
    rough = jax.random.uniform(second, (D, 1), jnp.float32, 0.7, 1.3)
    values = jnp.clip(jax.random.normal(first, (D, D), jnp.float32), -5.0, 5.0)
    ratio = 3.0
    scale = 0.6 * jnp.power(ratio, position)[:, None] * rough
    return (values * scale).astype(jnp.float32)


def strengthened(entries, rng, source, target, shards_of, factor):
    def block_of(axis_at):
        return (jnp.arange(entries.shape[axis_at]) // (entries.shape[axis_at] // shards_of)).reshape((-1,) + (1,) * (entries.ndim - 1 - axis_at))

    near = jax.random.permutation(rng, shards_of)[block_of(target)]
    second = (block_of(target) + shards_of // 2) % shards_of
    return jnp.where((block_of(source) == near) | (block_of(source) == second), factor * entries, entries)


def levels(key, shape, pieces, smallest, high):
    def one(dim, shards_of):
        draws = jax.random.uniform(jax.random.fold_in(jax.random.fold_in(key, 6), dim), (shards_of,), jnp.float32, smallest / len(pieces), high / len(pieces))
        return jnp.repeat(jnp.exp(draws), shape[dim] // shards_of).reshape((-1,) + (1,) * (len(shape) - dim - 1))

    factor_of = one(*pieces[0])
    for cut in pieces[1:]:
        factor_of = factor_of * one(*cut)
    return factor_of


def gaussian(key, dims, deviation, bound, split=(), kind=jnp.bfloat16):
    result = deviation * jax.random.normal(key, dims, jnp.float32)
    if split:
        result = result * levels(key, dims, split, -0.22, 0.18)
    return jnp.clip(result, -bound, bound).astype(kind)


def bell_draw_with(rng, dims, width, bound, cuts, heavy, held_as=jnp.bfloat16):
    array = width * jax.random.normal(rng, dims, jnp.float32)
    if cuts:
        array = array * levels(rng, dims, cuts, -0.22, 0.18)
    return jnp.clip(strengthened(array, jax.random.fold_in(rng, 3), *heavy), -bound, bound).astype(held_as)


def setup_inputs(seed: int = 0) -> dict:
    keys = jax.random.split(jax.random.key(seed), 4)
    return {
        "grad_parts": bell_draw_with(keys[0], (REPLICAS, D, D), 1.0, 6.0, ((0, 4), (1, 2), (2, 4)), (0, 1, 4, 2.0)),
        "momentum": draw_momentum(jax.random.fold_in(keys[3], 71), 0),
        "basis": gaussian(keys[2], (D, RANK), D ** -0.5, 0.0625, ((0, 4),), jnp.float32),
    }


EPS = 1e-06
FEEDBACK = 0.05
HIGH = lax.Precision.HIGHEST

def reference(grad_parts, momentum, basis):

    def add_part(total, part):
        return (total + part.astype(jnp.float32), None)
    total, _ = lax.scan(add_part, jnp.zeros((D, D), jnp.float32), grad_parts)
    blended = momentum + total / REPLICAS
    power = jnp.dot(blended, basis, precision=HIGH)
    squares = lax.optimization_barrier(jnp.sum(power * power, axis=0))
    power_norms = jnp.sqrt(squares / D)
    scaled = power / (jnp.sqrt(squares) + EPS)
    gram = jnp.dot(scaled.T, scaled, precision=HIGH)
    factor = jnp.linalg.cholesky(gram)
    orth = jax.scipy.linalg.solve_triangular(factor, scaled.T, lower=True).T
    back = jnp.dot(blended.T, orth, precision=HIGH)
    back_norms = jnp.sqrt(lax.optimization_barrier(jnp.sum(back * back, axis=0)))
    new_basis = back / (back_norms + EPS)
    new_momentum = blended - FEEDBACK * jnp.dot(orth, back.T, precision=HIGH)
    scale = D / RANK ** 0.5
    update = (scale * jnp.dot(orth, new_basis.T, precision=HIGH)).astype(jnp.bfloat16)
    return (update, new_momentum, new_basis, power_norms)
```

```python
import functools

import jax
import jax.numpy as jnp
from jax import lax
from jax.experimental import pallas as pl
from jax.experimental.pallas import tpu as pltpu
from jax.sharding import PartitionSpec as P


EPS = 1e-06
FEEDBACK = 0.05
HIGHEST = lax.Precision.HIGHEST
HIGH = lax.Precision.HIGH
F32 = jnp.float32
BF16 = jnp.bfloat16
BLOCK = 128
PANEL = 8


def dot(a, b, contract, precision=None):
    dims = (((contract[0],), (contract[1],)), ((), ()))
    return lax.dot_general(a, b, dims, precision=precision, preferred_element_type=F32)


def split(x):
    hi = x.astype(BF16)
    return hi, (x - hi.astype(F32)).astype(BF16)


def pick(x, k, axis=0):
    return lax.dynamic_index_in_dim(x, k, axis, keepdims=False, allow_negative_indices=False)


def strip(x, start, size, axis):
    return lax.dynamic_slice_in_dim(x, start, size, axis, allow_negative_indices=False)


def wrap(v, n):
    return v & (n - 1) if n & (n - 1) == 0 else lax.rem(v, n)


class Group:
    def __init__(self, axis, size, stride=1):
        self.axis, self.n, self.stride = axis, size, stride
        self.total = lax.axis_size(axis)
        self.me = wrap(lax.div(lax.axis_index(axis), stride), size)

    def shift(self, x, by):
        perm = []
        for i in range(self.total):
            digit = (i // self.stride) % self.n
            perm.append((i, i + ((digit + by) % self.n - digit) * self.stride))
        return lax.ppermute(x, self.axis, perm)

    def line_reduce_scatter(self, x):
        n = self.n
        if n == 4:
            return self.four_reduce_scatter(x)
        up = down = None
        for hop in range(n - 1):
            ends = range(hop + 1)
            far = n - 1 - hop

            def step(k, before, pairs):
                part = pick(x, wrap(self.me + k, n)).astype(F32)
                part = part if before is None else part + before.astype(F32)
                return lax.ppermute(part.astype(BF16), self.axis, pairs)

            up = step(far, up, [(i, i + 1) for i in ends])
            down = step(n - far, down, [(n - 1 - i, n - 2 - i) for i in ends])
        own = pick(x, self.me).astype(F32)
        return own + up.astype(F32) + down.astype(F32)

    def four_reduce_scatter(self, x):
        def part(k):
            return pick(x, wrap(self.me + k, 4)).astype(F32)

        two = part(2).astype(BF16)
        up = lax.ppermute(two, self.axis, [(0, 1), (1, 2)])
        down = lax.ppermute(two, self.axis, [(3, 2), (2, 1)])
        up = self.shift((part(1) + up.astype(F32)).astype(BF16), 1)
        down = self.shift((part(3) + down.astype(F32)).astype(BF16), 3)
        return part(0) + up.astype(F32) + down.astype(F32)

    def place(self, parts, axis=0):
        shape = parts[0].shape
        out = jnp.zeros(shape[:axis] + (self.n,) + shape[axis:], parts[0].dtype)
        for k, part in enumerate(parts):
            at = [0] * out.ndim
            at[axis] = wrap(self.me + self.n - k, self.n)
            part = jnp.expand_dims(part, axis)
            out = lax.dynamic_update_slice(out, part, at, allow_negative_indices=False)
        return out

    def gather_parts(self, x):
        return [x] + [self.shift(x, k) for k in range(1, self.n)]

    def line_gather_parts(self, x):
        parts = self.gather_parts(x) if self.n != 4 else [x, self.shift(x, 1), None, self.shift(x, 3)]
        if parts[2] is None:
            up = lax.ppermute(parts[1], self.axis, [(1, 2), (2, 3)])
            down = lax.ppermute(parts[3], self.axis, [(2, 1), (1, 0)])
            parts[2] = up + down
        return parts

    def all_sum(self, x):
        return functools.reduce(jnp.add, self.gather_parts(x))


def after(x, earlier):
    return lax.optimization_barrier((x, earlier))[0]


def power_kernel(reps, n, rank, at_ref, g_ref, m_ref, b_ref, out_ref, sum_ref):
    step = pl.program_id(0)
    both = b_ref[...]
    hi, lo = split(m_ref[...])
    rows = g_ref[...].reshape(reps * n, -1)
    cut = [slice(0, reps * n), slice(reps * n, (reps + 1) * n), slice((reps + 1) * n, (reps + 2) * n)]

    @pl.when(step == 0)
    def _():
        sum_ref[...] = jnp.zeros_like(sum_ref)

    sum_ref[cut[0], :] += dot(rows, both, (1, 0))
    sum_ref[cut[1], :] += dot(hi, both, (1, 0))
    sum_ref[cut[2], :rank] += dot(lo, both[:, :rank], (1, 0))

    @pl.when(step == pl.num_programs(0) - 1)
    def _():
        out = sum_ref[cut[0], :rank] + sum_ref[cut[0], rank:]
        out_ref[...] = out.reshape(reps, n, rank) * (1.0 / reps)
        mine = sum_ref[cut[1], :rank] + sum_ref[cut[1], rank:] + sum_ref[cut[2], :rank]
        out_ref[pl.ds(at_ref[1], 1)] += mine[None]


def power_rows(grads, momentum, both, block, rep, reps, n):
    width, rank = grads.shape[1], both.shape[1] // 2
    if n % 16:
        high, low = both[:, :rank], both[:, rank:]
        rows = pick(grads.reshape(reps, -1, n, width), block, 1)
        out = (dot(rows, high, (2, 0)) + dot(rows, low, (2, 0))) / reps
        mine = strip(momentum, block * n, n, 0)
        mine = dot(mine, high.astype(F32) + low.astype(F32), (1, 0), HIGH)
        here = lax.broadcasted_iota(jnp.int32, (reps, 1, 1), 0) == rep
        return jnp.where(here, out + mine, out)
    wide = 512 if width % 512 == 0 else width
    return pl.pallas_call(
        functools.partial(power_kernel, reps, n, rank),
        grid_spec=pltpu.PrefetchScalarGridSpec(
            num_scalar_prefetch=1,
            grid=(width // wide,),
            in_specs=[
                pl.BlockSpec((reps, 1, n, wide), lambda i, at: (0, at[0], 0, i)),
                pl.BlockSpec((n, wide), lambda i, at: (at[0], i)),
                pl.BlockSpec((wide, 2 * rank), lambda i, at: (i, 0)),
            ],
            out_specs=pl.BlockSpec((reps, n, rank), lambda i, at: (0, 0, 0)),
            scratch_shapes=[pltpu.VMEM(((reps + 2) * n, 2 * rank), F32)],
        ),
        out_shape=jax.ShapeDtypeStruct((reps, n, rank), F32),
        cost_estimate=pl.CostEstimate(
            flops=(reps + 2) * n * width * rank // 4,
            bytes_accessed=2 * (reps + 2) * n * width + 4 * width * rank + 4 * reps * n * rank,
            transcendentals=0,
        ),
        compiler_params=pltpu.CompilerParams(vmem_limit_bytes=56 * 2**20),
        name="power_rows",
    )(jnp.stack([block, rep]).astype(jnp.int32), grads.reshape(reps, -1, n, width), momentum, both)


def block_inverse(a):
    n = a.shape[0]
    row = lax.broadcasted_iota(jnp.int32, (n, n), 0)
    lane = lax.broadcasted_iota(jnp.int32, (n, n), 1)
    x = (row == lane).astype(F32)
    scale = jnp.ones((n, n), F32)
    for k in range(0, n, PANEL):
        cols = [jnp.broadcast_to(a[:, k + j : k + j + 1], (n, n)) for j in range(PANEL)]
        for j in range(PANEL):
            at = k + j
            pivot = cols[j][at : at + 1, :]
            step = jnp.where(row > at, cols[j] * (1.0 / pivot), 0.0)
            scale = jnp.where(row == at, lax.rsqrt(pivot), scale)
            a = a - step * a[at : at + 1, :]
            x = x - step * x[at : at + 1, :]
            for l in range(j + 1, PANEL):
                cols[l] = cols[l] - step * cols[l][at : at + 1, :]
    return x * scale


def factor_kernel(gram_ref, turn_ref, squares_ref):
    gram = gram_ref[...]
    n = gram.shape[0]
    row = lax.broadcasted_iota(jnp.int32, (n, n), 0)
    lane = lax.broadcasted_iota(jnp.int32, (n, n), 1)
    diag = jnp.where(row == lane, gram, 0.0)
    across = jnp.sum(diag, axis=0, keepdims=True)
    down = jnp.sum(diag, axis=1, keepdims=True)
    squares_ref[...] = jnp.broadcast_to(across, squares_ref.shape)
    inv_down = 1.0 / (jnp.sqrt(down) + EPS)
    a = gram * inv_down * (1.0 / (jnp.sqrt(across) + EPS))
    m = n // BLOCK
    cut = [slice(i * BLOCK, (i + 1) * BLOCK) for i in range(m)]
    left = {(i, j): a[cut[i], cut[j]] for i in range(m) for j in range(i, m)}
    inv = {}
    for k in range(m):
        one = block_inverse(left[k, k])
        right = {j: dot(one, left[k, j], (1, 0), HIGHEST) for j in range(k + 1, m)}
        for j in range(k):
            inv[k, j] = dot(one, inv[k, j], (1, 0), HIGHEST)
        inv[k, k] = one
        for i in range(k + 1, m):
            for j in range(i, m):
                left[i, j] = left[i, j] - dot(right[i], right[j], (0, 0), HIGHEST)
            for j in range(k + 1):
                d = dot(right[i], inv[k, j], (0, 0), HIGHEST)
                inv[i, j] = inv[i, j] - d if (i, j) in inv else -d
    for i in range(m):
        for j in range(m):
            if j <= i:
                turn_ref[cut[j], cut[i]] = jnp.swapaxes(inv[i, j], 0, 1) * inv_down[cut[j], :]
            else:
                turn_ref[cut[j], cut[i]] = jnp.zeros((BLOCK, BLOCK), F32)


def factor(gram):
    n = gram.shape[0]
    turn, squares = pl.pallas_call(
        factor_kernel,
        out_shape=(jax.ShapeDtypeStruct((n, n), F32), jax.ShapeDtypeStruct((8, n), F32)),
        cost_estimate=pl.CostEstimate(flops=10**9, bytes_accessed=12 * n * n, transcendentals=0),
        compiler_params=pltpu.CompilerParams(vmem_limit_bytes=16 * 2**20),
        name="factor",
    )(gram)
    return turn, squares[0]


def local(grad_parts, momentum, basis):
    reps, rows, cols = (lax.axis_size(a) for a in ("rep", "row", "col"))
    cores = 2 if cols % 2 == 0 else 1
    z = Group("rep", reps)
    x = Group("row", rows)
    y = Group("col", cols // cores, cores)
    core = Group("col", cores)
    grads = grad_parts[0]
    height, width = grads.shape
    rank = basis.shape[1]
    whole_rows = height * rows
    share = momentum.shape[0]
    n = share // cols
    at = z.me * share

    summed = lax.psum_scatter(grads, "rep", scatter_dimension=0, tiled=True)

    both = jnp.concatenate(split(basis), axis=1)
    got = []
    first = y.me
    for k in [*range(1, y.n), 0]:
        block = wrap(first + k, y.n) * core.n
        parts = None
        for c in range(core.n - 1, -1, -1):
            part = power_rows(grads, momentum, both, block + wrap(core.me + c, core.n), z.me, reps, n)
            part = core.shift(part, c) if c else part
            parts = part if parts is None else parts + part
        if k:
            sent = parts.astype(BF16)
            first = after(first, sent)
            parts = y.shift(sent, k).astype(F32)
        got.append(parts)
    own = z.line_reduce_scatter(functools.reduce(jnp.add, got)).astype(BF16)
    columns = z.line_gather_parts(own)
    chip = [z.place(columns)]
    chip += [z.place([y.shift(part, k) for part in columns]) for k in range(1, y.n)]
    sides = [y.place(chip, 1)] + [
        y.place([core.shift(part, c) for part in chip], 1) for c in range(1, core.n)
    ]
    power = core.place(sides, 2).reshape(height, rank)
    own_power = strip(power, at, share, 0)

    gram = dot(power, power, (0, 0))
    turn, squares = factor(x.all_sum(gram))
    power_norms = jnp.sqrt(squares / whole_rows)

    first = after(x.me, gram)

    def across(k):
        width_k = width // rows
        start = wrap(first + k, rows) * width_k
        g = strip(grads, start, width_k, 1)
        m = strip(momentum, start, width_k, 1)
        out = dot(g, power, (0, 0)) / reps + dot(m, own_power.astype(F32), (0, 0), HIGH)
        return out.reshape(reps, -1, rank)

    got = [x.shift(across(k).astype(BF16), k).astype(F32) for k in range(1, rows)]
    part = z.line_reduce_scatter(after(functools.reduce(jnp.add, got, across(0)), turn))

    own_back = dot(part, turn, (1, 0), HIGHEST).astype(BF16)
    columns = z.line_gather_parts(own_back)
    back = [z.place(columns)]
    back += [z.place([x.shift(part, k) for part in columns]) for k in range(1, rows)]
    back = x.place(back).reshape(width, rank)
    back_squares = y.all_sum(core.all_sum(jnp.sum(back.astype(F32) ** 2, axis=0)))
    own_orth = dot(own_power.astype(F32), turn, (1, 0), HIGH).astype(BF16)
    new_momentum = momentum + summed.astype(F32) / reps - FEEDBACK * dot(own_orth, back, (1, 1))
    new_basis = back.astype(F32) / (jnp.sqrt(back_squares) + EPS)
    scale = whole_rows / rank**0.5
    turned = (scale * dot(new_basis, turn, (1, 1), HIGH)).astype(BF16)
    update = dot(power, turned, (1, 1)).astype(BF16)
    return (update, new_momentum, new_basis, power_norms)


def solution(mesh):
    placed = (P("rep", "row", "col"), P(("row", "rep"), "col"), P("col", None))
    return jax.shard_map(
        local,
        mesh=mesh,
        in_specs=placed,
        out_specs=(P("row", "col"), P(("row", "rep"), "col"), P("col", None), P()),
        check_vma=False,
    )
```

```python
import functools

import jax
import jax.numpy as jnp
from jax import lax
from jax.experimental import pallas as pl
from jax.experimental.pallas import tpu as pltpu
from jax.sharding import PartitionSpec as P


EPS = 1e-06
FEEDBACK = 0.05
HIGHEST = lax.Precision.HIGHEST
HIGH = lax.Precision.HIGH
F32 = jnp.float32
BF16 = jnp.bfloat16
BLOCK = 128
PANEL = 8


def dot(a, b, contract, precision=None):
    dims = (((contract[0],), (contract[1],)), ((), ()))
    return lax.dot_general(a, b, dims, precision=precision, preferred_element_type=F32)


def split(x):
    hi = x.astype(BF16)
    return hi, (x - hi.astype(F32)).astype(BF16)


def pick(x, k, axis=0):
    return lax.dynamic_index_in_dim(x, k, axis, keepdims=False, allow_negative_indices=False)


def strip(x, start, size, axis):
    return lax.dynamic_slice_in_dim(x, start, size, axis, allow_negative_indices=False)


def wrap(v, n):
    return v & (n - 1) if n & (n - 1) == 0 else lax.rem(v, n)


class Group:
    def __init__(self, axis, size, stride=1):
        self.axis, self.n, self.stride = axis, size, stride
        self.total = lax.axis_size(axis)
        self.me = wrap(lax.div(lax.axis_index(axis), stride), size)

    def shift(self, x, by):
        perm = []
        for i in range(self.total):
            digit = (i // self.stride) % self.n
            perm.append((i, i + ((digit + by) % self.n - digit) * self.stride))
        return lax.ppermute(x, self.axis, perm)

    def line_reduce_scatter(self, x):
        n = self.n
        if n == 4:
            return self.four_reduce_scatter(x)
        up = down = None
        for hop in range(n - 1):
            ends = range(hop + 1)
            far = n - 1 - hop

            def step(k, before, pairs):
                part = pick(x, wrap(self.me + k, n)).astype(F32)
                part = part if before is None else part + before.astype(F32)
                return lax.ppermute(part.astype(BF16), self.axis, pairs)

            up = step(far, up, [(i, i + 1) for i in ends])
            down = step(n - far, down, [(n - 1 - i, n - 2 - i) for i in ends])
        own = pick(x, self.me).astype(F32)
        return own + up.astype(F32) + down.astype(F32)

    def four_reduce_scatter(self, x):
        def part(k):
            return pick(x, wrap(self.me + k, 4)).astype(F32)

        two = part(2).astype(BF16)
        up = lax.ppermute(two, self.axis, [(0, 1), (1, 2)])
        down = lax.ppermute(two, self.axis, [(3, 2), (2, 1)])
        up = self.shift((part(1) + up.astype(F32)).astype(BF16), 1)
        down = self.shift((part(3) + down.astype(F32)).astype(BF16), 3)
        return part(0) + up.astype(F32) + down.astype(F32)

    def place(self, parts, axis=0):
        shape = parts[0].shape
        out = jnp.zeros(shape[:axis] + (self.n,) + shape[axis:], parts[0].dtype)
        for k, part in enumerate(parts):
            at = [0] * out.ndim
            at[axis] = wrap(self.me + self.n - k, self.n)
            part = jnp.expand_dims(part, axis)
            out = lax.dynamic_update_slice(out, part, at, allow_negative_indices=False)
        return out

    def gather_parts(self, x):
        return [x] + [self.shift(x, k) for k in range(1, self.n)]

    def line_gather_parts(self, x):
        parts = self.gather_parts(x) if self.n != 4 else [x, self.shift(x, 1), None, self.shift(x, 3)]
        if parts[2] is None:
            up = lax.ppermute(parts[1], self.axis, [(1, 2), (2, 3)])
            down = lax.ppermute(parts[3], self.axis, [(2, 1), (1, 0)])
            parts[2] = up + down
        return parts

    def all_sum(self, x):
        return functools.reduce(jnp.add, self.gather_parts(x))


def after(x, earlier):
    return lax.optimization_barrier((x, earlier))[0]


def power_kernel(reps, n, rank, at_ref, g_ref, m_ref, b_ref, out_ref, sum_ref, both_ref):
    step = pl.program_id(0)
    both_ref[:, :rank], both_ref[:, rank:] = split(b_ref[...])
    both = both_ref[...]
    hi, lo = split(m_ref[...])
    rows = g_ref[...].reshape(reps * n, -1)
    cut = [slice(0, reps * n), slice(reps * n, (reps + 1) * n), slice((reps + 1) * n, (reps + 2) * n)]

    @pl.when(step == 0)
    def _():
        sum_ref[...] = jnp.zeros_like(sum_ref)

    sum_ref[cut[0], :] += dot(rows, both, (1, 0))
    sum_ref[cut[1], :] += dot(hi, both, (1, 0))
    sum_ref[cut[2], :rank] += dot(lo, both[:, :rank], (1, 0))

    @pl.when(step == pl.num_programs(0) - 1)
    def _():
        out = sum_ref[cut[0], :rank] + sum_ref[cut[0], rank:]
        out_ref[...] = out.reshape(reps, n, rank) * (1.0 / reps)
        mine = sum_ref[cut[1], :rank] + sum_ref[cut[1], rank:] + sum_ref[cut[2], :rank]
        out_ref[pl.ds(at_ref[1], 1)] += mine[None]


def power_rows(grads, momentum, basis, block, rep, reps, n):
    width, rank = grads.shape[1], basis.shape[1]
    if n % 16:
        high, low = split(basis)
        rows = pick(grads.reshape(reps, -1, n, width), block, 1)
        out = (dot(rows, high, (2, 0)) + dot(rows, low, (2, 0))) / reps
        mine = strip(momentum, block * n, n, 0)
        mine = dot(mine, basis, (1, 0), HIGH)
        here = lax.broadcasted_iota(jnp.int32, (reps, 1, 1), 0) == rep
        return jnp.where(here, out + mine, out)
    wide = 512 if width % 512 == 0 else width
    return pl.pallas_call(
        functools.partial(power_kernel, reps, n, rank),
        grid_spec=pltpu.PrefetchScalarGridSpec(
            num_scalar_prefetch=1,
            grid=(width // wide,),
            in_specs=[
                pl.BlockSpec((reps, 1, n, wide), lambda i, at: (0, at[0], 0, i)),
                pl.BlockSpec((n, wide), lambda i, at: (at[0], i)),
                pl.BlockSpec((wide, rank), lambda i, at: (i, 0)),
            ],
            out_specs=pl.BlockSpec((reps, n, rank), lambda i, at: (0, 0, 0)),
            scratch_shapes=[pltpu.VMEM(((reps + 2) * n, 2 * rank), F32), pltpu.VMEM((wide, 2 * rank), BF16)],
        ),
        out_shape=jax.ShapeDtypeStruct((reps, n, rank), F32),
        cost_estimate=pl.CostEstimate(
            flops=(reps + 2) * n * width * rank // 4,
            bytes_accessed=2 * (reps + 2) * n * width + 4 * width * rank + 4 * reps * n * rank,
            transcendentals=0,
        ),
        compiler_params=pltpu.CompilerParams(vmem_limit_bytes=56 * 2**20),
        name="power_rows",
    )(jnp.stack([block, rep]).astype(jnp.int32), grads.reshape(reps, -1, n, width), momentum, basis)


def block_inverse(a):
    n = a.shape[0]
    row = lax.broadcasted_iota(jnp.int32, (n, n), 0)
    lane = lax.broadcasted_iota(jnp.int32, (n, n), 1)
    x = (row == lane).astype(F32)
    scale = jnp.ones((n, n), F32)
    for k in range(0, n, PANEL):
        cols = [jnp.broadcast_to(a[:, k + j : k + j + 1], (n, n)) for j in range(PANEL)]
        for j in range(PANEL):
            at = k + j
            pivot = cols[j][at : at + 1, :]
            step = jnp.where(row > at, cols[j] * (1.0 / pivot), 0.0)
            scale = jnp.where(row == at, lax.rsqrt(pivot), scale)
            a = a - step * a[at : at + 1, :]
            x = x - step * x[at : at + 1, :]
            for l in range(j + 1, PANEL):
                cols[l] = cols[l] - step * cols[l][at : at + 1, :]
    return x * scale


def factor_kernel(gram_ref, turn_ref, squares_ref, left_ref, inv_ref):
    gram = gram_ref[...]
    n = gram.shape[0]
    row = lax.broadcasted_iota(jnp.int32, (n, n), 0)
    lane = lax.broadcasted_iota(jnp.int32, (n, n), 1)
    diag = jnp.where(row == lane, gram, 0.0)
    across = jnp.sum(diag, axis=0, keepdims=True)
    down = jnp.sum(diag, axis=1, keepdims=True)
    squares_ref[...] = jnp.broadcast_to(across, squares_ref.shape)
    inv_across = 1.0 / (jnp.sqrt(across) + EPS)
    left_ref[...] = gram * (1.0 / (jnp.sqrt(down) + EPS)) * inv_across
    inv_ref[...] = (row == lane).astype(F32)

    def block(k, carry):
        at = pl.multiple_of(k * BLOCK, BLOCK)
        here = pl.ds(at, BLOCK)
        one = block_inverse(left_ref[here, here])
        right = dot(one, left_ref[here, :], (1, 0), HIGHEST)
        beyond = lax.broadcasted_iota(jnp.int32, right.shape, 1) >= at + BLOCK
        right = jnp.where(beyond, right, 0.0)
        mine = dot(one, inv_ref[here, :], (1, 0), HIGHEST)
        inv_ref[here, :] = mine
        for i in range(1, n // BLOCK):
            rows = slice(i * BLOCK, (i + 1) * BLOCK)
            both = dot(right[:, rows], jnp.concatenate([right, mine], axis=1), (0, 0), HIGHEST)
            left_ref[rows, :] -= both[:, :n]
            inv_ref[rows, :] -= both[:, n:]
        return carry

    lax.fori_loop(0, n // BLOCK, block, 0)
    turn_ref[...] = jnp.swapaxes(inv_ref[...] * inv_across, 0, 1)


def factor(gram):
    n = gram.shape[0]
    turn, squares = pl.pallas_call(
        factor_kernel,
        out_shape=(jax.ShapeDtypeStruct((n, n), F32), jax.ShapeDtypeStruct((8, n), F32)),
        scratch_shapes=[pltpu.VMEM((n, n), F32)] * 2,
        cost_estimate=pl.CostEstimate(flops=10**9, bytes_accessed=12 * n * n, transcendentals=0),
        compiler_params=pltpu.CompilerParams(vmem_limit_bytes=16 * 2**20),
        name="factor",
    )(gram)
    return turn, squares[0]


def across_kernel(reps, steps, at_ref, g_ref, m_ref, p_ref, out_ref, sum_ref):
    step = pl.program_id(0)
    power = p_ref[...]

    @pl.when(step == 0)
    def _():
        sum_ref[...] = jnp.zeros_like(sum_ref)

    @pl.when(step < steps)
    def _():
        sum_ref[...] += dot(power, g_ref[...], (0, 0))

    @pl.when(step == steps)
    def _():
        sum_ref[...] = sum_ref[...] * (1.0 / reps)

    @pl.when(step >= steps)
    def _():
        hi, lo = split(m_ref[...])
        sum_ref[...] += dot(power, hi, (0, 0)) + dot(power, lo, (0, 0))

    @pl.when(step == pl.num_programs(0) - 1)
    def _():
        out_ref[...] = jnp.swapaxes(sum_ref[...], 0, 1)


def across(grads, momentum, power, k, rep, reps, rows):
    height, width = grads.shape
    share, rank = momentum.shape[0], power.shape[1]
    wide = width // rows
    deep = min(1024, share)
    if wide % 128:
        g, m = strip(grads, k * wide, wide, 1), strip(momentum, k * wide, wide, 1)
        mine = strip(power, rep * share, share, 0).astype(F32)
        return dot(g, power, (0, 0)) / reps + dot(m, mine, (0, 0), HIGH)
    steps, extra = height // deep, share // deep
    return pl.pallas_call(
        functools.partial(across_kernel, reps, steps),
        grid_spec=pltpu.PrefetchScalarGridSpec(
            num_scalar_prefetch=1,
            grid=(steps + extra,),
            in_specs=[
                pl.BlockSpec((deep, wide), lambda i, at: (jnp.minimum(i, steps - 1), at[0])),
                pl.BlockSpec((deep, wide), lambda i, at: (jnp.maximum(i - steps, 0), at[0])),
                pl.BlockSpec(
                    (deep, rank),
                    lambda i, at: (jnp.where(i < steps, i, at[1] * extra + i - steps), 0),
                ),
            ],
            out_specs=pl.BlockSpec((wide, rank), lambda i, at: (0, 0)),
            scratch_shapes=[pltpu.VMEM((rank, wide), F32)],
        ),
        out_shape=jax.ShapeDtypeStruct((wide, rank), F32),
        cost_estimate=pl.CostEstimate(
            flops=(height + 2 * share) * wide * rank // 2,
            bytes_accessed=2 * (height + 2 * share) * wide,
            transcendentals=0,
        ),
        compiler_params=pltpu.CompilerParams(vmem_limit_bytes=56 * 2**20),
        name="across",
    )(jnp.stack([k, rep]).astype(jnp.int32), grads, momentum, power)


def turn_kernel(scale, rank, b_ref, t_ref, out_ref):
    (b_hi, b_lo), (t_hi, t_lo) = split(b_ref[...]), split(t_ref[...])
    out = dot(b_hi, t_hi, (1, 1)) + dot(b_hi, t_lo, (1, 1)) + dot(b_lo, t_hi, (1, 1))
    out_ref[:, :rank], out_ref[:, rank:] = split(scale * out)


def turned_rows(basis, turn, scale):
    width, rank = basis.shape
    n = min(512, width)
    return pl.pallas_call(
        functools.partial(turn_kernel, scale, rank),
        grid=(width // n,),
        in_specs=[pl.BlockSpec((n, rank), lambda i: (i, 0)), pl.BlockSpec(turn.shape, lambda i: (0, 0))],
        out_specs=pl.BlockSpec((n, 2 * rank), lambda i: (i, 0)),
        out_shape=jax.ShapeDtypeStruct((width, 2 * rank), BF16),
        cost_estimate=pl.CostEstimate(
            flops=2 * width * rank * rank, bytes_accessed=8 * width * rank, transcendentals=0
        ),
        compiler_params=pltpu.CompilerParams(vmem_limit_bytes=56 * 2**20),
        name="turned_rows",
    )(basis, turn)


def update_kernel(rank, p_ref, q_ref, out_ref, twice_ref):
    power = p_ref[...]
    twice_ref[:, :rank], twice_ref[:, rank:] = power, power
    out_ref[...] = dot(twice_ref[...], q_ref[...], (1, 1)).astype(BF16)


def update_rows(power, turned):
    height, rank = power.shape
    width = turned.shape[0]
    n = min(1024, height)
    return pl.pallas_call(
        functools.partial(update_kernel, rank),
        grid=(height // n,),
        in_specs=[
            pl.BlockSpec((n, rank), lambda i: (i, 0)),
            pl.BlockSpec(turned.shape, lambda i: (0, 0)),
        ],
        out_specs=pl.BlockSpec((n, width), lambda i: (i, 0)),
        scratch_shapes=[pltpu.VMEM((n, 2 * rank), BF16)],
        out_shape=jax.ShapeDtypeStruct((height, width), BF16),
        cost_estimate=pl.CostEstimate(
            flops=height * width * rank, bytes_accessed=2 * height * width, transcendentals=0
        ),
        compiler_params=pltpu.CompilerParams(vmem_limit_bytes=56 * 2**20),
        name="update_rows",
    )(power, turned)


def feed_kernel(reps, m_ref, s_ref, orth_ref, back_ref, out_ref):
    given = FEEDBACK * dot(orth_ref[...], back_ref[...], (1, 1))
    out_ref[...] = m_ref[...] + s_ref[...].astype(F32) * (1.0 / reps) - given


def feed_back(momentum, summed, orth, back, reps):
    share, width = momentum.shape
    rank = orth.shape[1]
    n = min(256, share)
    rows = pl.BlockSpec((n, width), lambda i: (i, 0))
    return pl.pallas_call(
        functools.partial(feed_kernel, reps),
        grid=(share // n,),
        in_specs=[
            rows,
            rows,
            pl.BlockSpec((n, rank), lambda i: (i, 0)),
            pl.BlockSpec((width, rank), lambda i: (0, 0)),
        ],
        out_specs=rows,
        out_shape=jax.ShapeDtypeStruct(momentum.shape, F32),
        cost_estimate=pl.CostEstimate(
            flops=2 * share * width * rank, bytes_accessed=10 * share * width, transcendentals=0
        ),
        compiler_params=pltpu.CompilerParams(vmem_limit_bytes=56 * 2**20),
        name="feed_back",
    )(momentum, summed, orth, back)


def local(grad_parts, momentum, basis):
    reps, rows, cols = (lax.axis_size(a) for a in ("rep", "row", "col"))
    cores = 2 if cols % 2 == 0 else 1
    z = Group("rep", reps)
    x = Group("row", rows)
    y = Group("col", cols // cores, cores)
    core = Group("col", cores)
    grads = grad_parts[0]
    height, width = grads.shape
    rank = basis.shape[1]
    whole_rows = height * rows
    share = momentum.shape[0]
    n = share // cols
    at = z.me * share

    summed = lax.psum_scatter(grads, "rep", scatter_dimension=0, tiled=True)

    got = []
    first = y.me
    for k in [*range(1, y.n), 0]:
        block = wrap(first + k, y.n) * core.n
        parts = None
        for c in range(core.n - 1, -1, -1):
            part = power_rows(grads, momentum, basis, block + wrap(core.me + c, core.n), z.me, reps, n)
            part = core.shift(part, c) if c else part
            parts = part if parts is None else parts + part
        if k:
            sent = parts.astype(BF16)
            first = after(first, sent)
            parts = y.shift(sent, k).astype(F32)
        got.append(parts)
    own = z.line_reduce_scatter(functools.reduce(jnp.add, got)).astype(BF16)
    columns = z.line_gather_parts(own)
    chip = [z.place(columns)]
    chip += [z.place([y.shift(part, k) for part in columns]) for k in range(1, y.n)]
    sides = [y.place(chip, 1)] + [
        y.place([core.shift(part, c) for part in chip], 1) for c in range(1, core.n)
    ]
    power = core.place(sides, 2).reshape(height, rank)
    own_power = strip(power, at, share, 0)

    gram = dot(power, power, (0, 0))
    total = x.all_sum(gram)
    turn, squares = factor(total)
    power_norms = jnp.sqrt(squares / whole_rows)

    first = after(x.me, gram)

    def piece(k):
        out = across(grads, momentum, power, wrap(first + k, rows), z.me, reps, rows)
        return out.reshape(reps, -1, rank)

    got = [x.shift(piece(k).astype(BF16), k).astype(F32) for k in range(1, rows)]
    part = z.line_reduce_scatter(after(functools.reduce(jnp.add, got, piece(0)), turn))

    own_back = dot(part, turn, (1, 0), HIGH).astype(BF16)
    back_squares = z.gather_parts(jnp.sum(own_back.astype(F32) ** 2, axis=0, keepdims=True))
    columns = z.line_gather_parts(own_back)
    back_squares = functools.reduce(jnp.add, after(back_squares, columns[1]))
    back_squares = x.all_sum(y.all_sum(core.all_sum(back_squares)))
    back = [z.place(columns)]
    back += [z.place([x.shift(part, k) for part in columns]) for k in range(1, rows)]
    back = x.place(back).reshape(width, rank)
    own_orth = dot(own_power, turn.astype(BF16), (1, 0)).astype(BF16)
    new_basis = back.astype(F32) / (jnp.sqrt(back_squares) + EPS)
    scale = whole_rows / rank**0.5
    turned = turned_rows(new_basis, turn, scale)
    update = update_rows(power, turned)
    new_momentum = feed_back(momentum, summed, own_orth, back, reps)
    return (update, new_momentum, new_basis, power_norms)


def solution(mesh):
    placed = (P("rep", "row", "col"), P(("row", "rep"), "col"), P("col", None))
    return jax.shard_map(
        local,
        mesh=mesh,
        in_specs=placed,
        out_specs=(P("row", "col"), P(("row", "rep"), "col"), P("col", None), P()),
        check_vma=False,
    )
```
